32 devices in a mesh: dp: 4 (over z), section: 2 (over core), space: 4 (over y, x).
Axes of the slice: x: 2, y: 2, z: 4, core: 2. Of those that a mesh axis runs over, the one named last changes fastest.
Arguments:
- latents: bfloat16 [16, 96, 192, 320], P('dp', 'space'), parts along dimension 0, may hold values from -16 to 16
- kernels: bfloat16 [2, 3, 3, 320, 320], P('section'), may hold values from -0.109375 to 0.109375
- norm_gain: float32 [2, 320], P('section'), may hold values from 0.25 to 1.75
- norm_bias: float32 [2, 320], P('section'), may hold values from -3 to 3
- conv_bias: float32 [2, 320], P('section'), may hold values from -3 to 3
Outputs:
- skips: bfloat16 [2, 16, 96, 192, 320], P('section', 'dp', 'space'), parts along dimension 1
The draws below stay inside these ranges and needn't reach their ends.
There are 4 independent parts, one for each index of `dp`. The reference program is written for one: setup_inputs(seed, part) draws one part's arguments, and reference() takes and returns one part's arrays. A program takes and returns all parts, laid end to end along the dimension named above; an argument that names none is the same for every part. Nothing has to cross between parts.
All inputs are finite; a program needn't handle non-finite values.
Results may differ from the reference program's by a relative error of at most 0.01.
Values may be sent and summed in bfloat16 or wider, within the bound.
A program may use at most 128 MiB of HBM per device.

```python
import jax
import jax.numpy as jnp
from jax import lax

C = 320
GROUPS = 32
H = 96
W = 192
MICRO = 4
SECTIONS = 2


def draw_latents(key, part):
    noise_key = jax.random.fold_in(key, 101)
    offset_key = jax.random.fold_in(key, 202)
    positions = jnp.arange(H, dtype=jnp.float32) / (H - 1)
    base = jax.random.normal(noise_key, (MICRO, H, W, C), jnp.float32)
    scales = 0.4 * jnp.exp(jnp.log(3.0) * positions)
    ramp = 0.3 * jnp.exp(jnp.log(10.0) * positions)
    offsets = 0.6 * jax.random.normal(offset_key, (MICRO, 1, 1, C), jnp.float32) + 1.0
    values = base * scales[None, :, None, None] + offsets * ramp[None, :, None, None]
    return jnp.clip(values, -16.0, 16.0).astype(jnp.bfloat16)


def block_levels(stream_key, dims, shards, least, largest):
    level, own = 1.0, jax.random.fold_in(stream_key, 6)
    for axis_at, shards_of in shards:
        heights = jnp.exp(jax.random.uniform(jax.random.fold_in(own, axis_at), (shards_of,), jnp.float32, least / len(shards), largest / len(shards)))
        level = level * jnp.repeat(heights, dims[axis_at] // shards_of).reshape([-1 if axis == axis_at else 1 for axis in range(len(dims))])
    return level


def gaussian(key, dims, scale, reach, cuts=(), held_as=jnp.bfloat16):
    level = block_levels(key, dims, cuts, -0.22, 0.18) if cuts else 1.0
    result = jax.random.normal(key, dims, jnp.float32) * scale * level
    return jnp.minimum(jnp.maximum(result, -reach), reach).astype(held_as)


def setup_inputs(seed: int = 0, part: int = 0) -> dict:
    splits = jax.random.split(jax.random.key(seed), 6)
    own_keys = jax.random.split(jax.random.fold_in(splits[5], part), 6)
    return {
        "latents": draw_latents(jax.random.fold_in(jax.random.fold_in(splits[5], part), 71), part),
        "kernels": gaussian(splits[1], (SECTIONS, 3, 3, C, C), (9 * C) ** -0.5, 0.109375, ((0, 2),)),
        "norm_gain": jnp.clip(1.0 + 0.15 * jax.random.normal(splits[2], (SECTIONS, C), jnp.float32), 0.25, 1.75),
        "norm_bias": gaussian(splits[3], (SECTIONS, C), 0.5, 3.0, ((0, 2),), jnp.float32),
        "conv_bias": gaussian(splits[4], (SECTIONS, C), 0.5, 3.0, ((0, 2),), jnp.float32),
    }


def group_norm_silu(inputs, norm_gain, norm_shift):
    batch_count = inputs.shape[0]
    values = inputs.astype(jnp.float32).reshape(batch_count, H * W, GROUPS, C // GROUPS)
    group_mean = lax.optimization_barrier(jnp.mean(values, axis=(1, 3), keepdims=True))
    deviation = values - group_mean
    group_var = lax.optimization_barrier(jnp.mean(deviation * deviation, axis=(1, 3), keepdims=True))
    scaled = (deviation * lax.rsqrt(group_var + 1e-05)).reshape(batch_count, H, W, C)
    scaled = scaled * norm_gain + norm_shift
    return jax.nn.silu(scaled).astype(jnp.bfloat16)

def convolve(normed, kernel):
    return lax.conv_general_dilated(normed, kernel, (1, 1), ((1, 1), (1, 1)), dimension_numbers=('NHWC', 'HWIO', 'NHWC'), preferred_element_type=jnp.float32)

def reference(latents, kernels, norm_gain, norm_bias, conv_bias):
    normed_first = group_norm_silu(latents, norm_gain[0], norm_bias[0])
    first = (convolve(normed_first, kernels[0]) + conv_bias[0]).astype(jnp.bfloat16)
    normed_second = group_norm_silu(first, norm_gain[1], norm_bias[1])
    second = (latents.astype(jnp.float32) + convolve(normed_second, kernels[1]) + conv_bias[1]).astype(jnp.bfloat16)
    return jnp.stack([first, second])
```

```python
import functools

import jax
import jax.numpy as jnp
from jax import lax
from jax.experimental import pallas as pl
from jax.experimental.pallas import tpu as pltpu
from jax.sharding import PartitionSpec as P

GROUPS = 32
EPS = 1e-05
MAIN = 256
VMEM_LIMIT = 60 * 1024 * 1024


def pick_block(rows):
    return max(d for d in range(1, 9) if rows % d == 0)


def column_pieces(channels):
    main = channels // MAIN * MAIN
    tail = channels - main
    return main, tail, 3 * main


def packed_width(channels):
    return -(-3 * channels // MAIN) * MAIN


def pack_kernel(k_ref, w_ref, buf):
    channels = k_ref.shape[-1]
    main, tail, base = column_pieces(channels)
    buf[...] = jnp.zeros_like(buf)
    for dr in range(3):
        for dc in range(3):
            tap = k_ref[dr, dc]
            for klo, khi, kdst in ((0, main, dc * main), (main, channels, base + dc * tail)):
                for nlo, nhi, ndst in ((0, main, dr * main), (main, channels, base + dr * tail)):
                    buf[kdst:kdst + khi - klo, ndst:ndst + nhi - nlo] = tap[klo:khi, nlo:nhi]
    w_ref[...] = buf[...]


def pack_weights(kernel):
    channels = kernel.shape[-1]
    width = packed_width(channels)
    return pl.pallas_call(
        pack_kernel,
        out_shape=jax.ShapeDtypeStruct((width, width), jnp.bfloat16),
        scratch_shapes=[pltpu.VMEM((width, width), jnp.bfloat16)],
        compiler_params=pltpu.CompilerParams(vmem_limit_bytes=VMEM_LIMIT),
        cost_estimate=pl.CostEstimate(flops=0, bytes_accessed=6 * width * width, transcendentals=0),
        name="pack",
    )(kernel)


def row_moments(values):
    mean = jnp.sum(values, axis=0, keepdims=True) * (1.0 / values.shape[0])
    deviation = values - mean
    return mean, jnp.sum(deviation * deviation, axis=0, keepdims=True)


def moments_kernel(scal, x_ref, m_ref):
    for i in range(x_ref.shape[1]):
        mean, spread = row_moments(x_ref[0, i].astype(jnp.float32))
        m_ref[0, 0, 0, i:i + 1, :] = mean
        m_ref[0, 1, 0, i:i + 1, :] = spread


def moments(scal, latents, count):
    _, rows, columns, channels = latents.shape
    block = pick_block(rows)
    return pl.pallas_call(
        moments_kernel,
        grid_spec=pltpu.PrefetchScalarGridSpec(
            num_scalar_prefetch=1,
            grid=(count, rows // block),
            in_specs=[
                pl.BlockSpec((1, block, columns, channels), lambda s, c, scal: (scal[3] + s, c, 0, 0))
            ],
            out_specs=pl.BlockSpec((1, 2, 1, block, channels), lambda s, c, scal: (s, 0, c, 0, 0)),
        ),
        out_shape=jax.ShapeDtypeStruct((count, 2, rows // block, block, channels), jnp.float32),
        compiler_params=pltpu.CompilerParams(vmem_limit_bytes=VMEM_LIMIT),
        cost_estimate=pl.CostEstimate(
            flops=0, bytes_accessed=count * rows * columns * channels * 2, transcendentals=0
        ),
        name="moments",
    )(scal, latents)


def conv_kernel(stage, parts, *refs):
    scal, x_ref, top_ref, bot_ref = refs[:4]
    stat_refs = refs[4:4 + parts]
    par_ref, wa_ref, wb_ref = refs[4 + parts:7 + parts]
    rest = refs[7 + parts:]
    if stage == 0:
        y_ref, m_ref = rest[:2]
        rest = rest[2:]
    else:
        if len(rest) > 13:
            rest_in, rest = rest[:3], rest[3:]
        else:
            rest_in, rest = rest[:2], rest[2:]
        res_ref, own_ref = rest_in[:2]
        keep_ref, y_ref = rest[:2]
        rest = rest[2:]
    w_ref, act_ref, lhs_a, lhs_b, p_ref, carry_ref, next_ref, ab_ref, sem = rest
    step, last = pl.program_id(0), pl.num_programs(0) - 1
    block, columns, channels = x_ref.shape[1:]
    main, tail, base = column_pieces(channels)
    width = w_ref.shape[0]
    unit = -(-block // 2)

    @pl.when(step == 0)
    def _():
        own_first = scal[0] == stage
        copy_a = pltpu.make_async_copy(wa_ref, w_ref, sem.at[0])
        copy_b = pltpu.make_async_copy(wb_ref, w_ref, sem.at[0])

        @pl.when(own_first)
        def _():
            copy_a.start()

        @pl.when(jnp.logical_not(own_first))
        def _():
            copy_b.start()

        act_ref[:, 0:8, :] = jnp.zeros((act_ref.shape[0], 8, channels), jnp.float32)
        act_ref[:, columns + 8:columns + 16, :] = jnp.zeros((act_ref.shape[0], 8, channels), jnp.float32)
        per_group = channels // GROUPS
        row_id = lax.broadcasted_iota(jnp.int32, (channels, channels), 0).astype(jnp.float32)
        col_id = lax.broadcasted_iota(jnp.int32, (channels, channels), 1).astype(jnp.float32)
        same = jnp.floor((row_id + 0.5) * (1.0 / per_group)) == jnp.floor((col_id + 0.5) * (1.0 / per_group))
        members = jnp.where(same, 1.0, 0.0).astype(jnp.float32)

        def over_groups(value):
            return jnp.dot(
                jnp.broadcast_to(value, (8, channels)), members,
                precision=lax.Precision.HIGHEST, preferred_element_type=jnp.float32,
            )[0:1]

        chunks, rows_of = stat_refs[0].shape[-3:-1]
        cells = parts * chunks * rows_of
        total = jnp.zeros((1, channels), jnp.float32)
        for ref in stat_refs:
            for j in range(chunks):
                total += jnp.sum(ref[0, 0, j], axis=0, keepdims=True)
        mean = over_groups(total) * (1.0 / (cells * per_group))
        spread = jnp.zeros((1, channels), jnp.float32)
        for ref in stat_refs:
            for j in range(chunks):
                away = ref[0, 0, j] - mean
                spread += jnp.sum(away * away * float(columns) + ref[0, 1, j], axis=0, keepdims=True)
        var = over_groups(spread) * (1.0 / (cells * per_group * columns))
        inv = lax.rsqrt(var + EPS)
        ab_ref[0:1, :] = mean
        ab_ref[1:2, :] = 0.5 * inv * par_ref[0:1, :]
        ab_ref[2:3, :] = 0.5 * par_ref[1:2, :]
        copy_a.wait()

    def activate(values, slot, lhs, place, valid=None):
        half = (values.astype(jnp.float32) - ab_ref[0:1, :]) * ab_ref[1:2, :] + ab_ref[2:3, :]
        act = half + half * jnp.tanh(half)
        if valid is not None:
            act = jnp.where(valid, act, 0.0)
        act_ref[slot, 8:columns + 8, :] = act
        rows = slice(place * columns, (place + 1) * columns)
        for dc in range(3):
            lhs[rows, dc * main:(dc + 1) * main] = act_ref[slot, 7 + dc:7 + dc + columns, 0:main].astype(jnp.bfloat16)
        tails = [act_ref[slot, 7 + dc:7 + dc + columns, main:channels] for dc in range(3)]
        tails.append(jnp.zeros((columns, width - base - 3 * tail), jnp.float32))
        lhs[rows, base:width] = jnp.concatenate(tails, axis=1).astype(jnp.bfloat16)

    def edge(ref, valid, tap, dst):
        activate(ref[...], 0, lhs_a, 0, valid)
        left = lhs_a[0:columns, :]
        dst[:, 0:main] = jnp.dot(left, w_ref[:, tap * main:(tap + 1) * main], preferred_element_type=jnp.float32)
        ends = jnp.dot(left, w_ref[:, base:width], preferred_element_type=jnp.float32)
        dst[:, main:channels] = ends[:, tap * tail:(tap + 1) * tail]

    @pl.when(step == 0)
    def _():
        edge(top_ref, scal[1] == 1, 0, carry_ref)

    @pl.when(step == last)
    def _():
        edge(bot_ref, scal[2] == 1, 2, next_ref)

    now = step % 2
    before = 1 - now

    @pl.when(step < last)
    def _():
        for u, lhs in ((0, lhs_a), (1, lhs_b)):
            lo, hi = u * unit, min((u + 1) * unit, block)
            if hi <= lo:
                continue
            for i in range(lo, hi):
                activate(x_ref[0, i], i, lhs, i - lo)
            p_ref[now, lo * columns:hi * columns, :] = jnp.dot(
                lhs[0:(hi - lo) * columns, :], w_ref[...], preferred_element_type=jnp.float32
            )
        next_ref[:, 0:main] = p_ref[now, 0:columns, 2 * main:3 * main]
        next_ref[:, main:channels] = p_ref[now, 0:columns, base + 2 * tail:base + 3 * tail]

    @pl.when(step > 0)
    def _():
        shift = par_ref[2:3, :]

        def tap_of(i, tap):
            rows = slice(i * columns, (i + 1) * columns)
            return (
                p_ref[before, rows, tap * main:(tap + 1) * main],
                p_ref[before, rows, base + tap * tail:base + (tap + 1) * tail],
            )

        def whole(ref):
            return ref[:, 0:main], ref[:, main:channels]

        for i in range(block):
            above = whole(carry_ref) if i == 0 else tap_of(i - 1, 0)
            middle = tap_of(i, 1)
            below = whole(next_ref) if i == block - 1 else tap_of(i + 1, 2)
            for j, (lo, hi) in enumerate(((0, main), (main, channels))):
                total = above[j] + middle[j] + below[j] + shift[:, lo:hi]
                if stage == 1:
                    total = total + res_ref[0, i, :, lo:hi].astype(jnp.float32)
                rounded = total.astype(jnp.bfloat16)
                y_ref[0, i, :, lo:hi] = rounded
                if stage == 0:
                    mean, spread = row_moments(rounded.astype(jnp.float32))
                    m_ref[0, 0, 0, i:i + 1, lo:hi] = mean
                    m_ref[0, 1, 0, i:i + 1, lo:hi] = spread
        if stage == 1:
            @pl.when(scal[0] == 0)
            def _():
                keep_ref[...] = own_ref[...]

            @pl.when(scal[0] != 0)
            def _():
                keep_ref[...] = y_ref[...]
        carry_ref[:, 0:main] = p_ref[before, (block - 1) * columns:block * columns, 0:main]
        carry_ref[:, main:channels] = p_ref[before, (block - 1) * columns:block * columns, base:base + tail]


def conv(stage, sample, scal, source, top, bottom, stats, params, own, other, latents=None, out=None):
    rows, columns, channels = source.shape[1:]
    block = pick_block(rows)
    chunks = rows // block
    width = packed_width(channels)
    unit = -(-block // 2)
    tile = (1, block, columns, channels)
    lag = lambda c: jnp.maximum(c - 1, 0)
    ahead = lambda c: jnp.minimum(c, chunks - 1)
    full = lambda a: pl.BlockSpec(a.shape, lambda c, scal, n=a.ndim: (0,) * n)
    anywhere = pl.BlockSpec(memory_space=pl.ANY)
    if stage == 0:
        main_spec = pl.BlockSpec(tile, lambda c, scal: (scal[3] + sample, ahead(c), 0, 0))
    else:
        main_spec = pl.BlockSpec(tile, lambda c, scal: (0, ahead(c), 0, 0))
    args = [source, top, bottom, *stats, params, own, other]
    in_specs = [main_spec, full(top), full(bottom), *[
        pl.BlockSpec((1,) + s.shape[1:], lambda c, scal: ((sample if stage == 0 else 0), 0, 0, 0, 0)) for s in stats
    ], full(params), anywhere, anywhere]
    plain = jax.ShapeDtypeStruct((1, rows, columns, channels), jnp.bfloat16)
    plain_spec = pl.BlockSpec(tile, lambda c, scal: (0, lag(c), 0, 0))
    aliases = {}
    if stage == 0:
        out_shape = (plain, jax.ShapeDtypeStruct((1, 2, chunks, block, channels), jnp.float32))
        out_specs = (plain_spec, pl.BlockSpec((1, 2, 1, block, channels), lambda c, scal: (0, 0, lag(c), 0, 0)))
    else:
        placed = pl.BlockSpec(tile, lambda c, scal: (scal[3] + sample, lag(c), 0, 0))
        args += [latents, source]
        in_specs += [placed, plain_spec]
        if out is not None:
            args.append(out)
            in_specs.append(anywhere)
            aliases = {len(args): 0}
        out_shape = (jax.ShapeDtypeStruct(latents.shape, jnp.bfloat16), plain)
        out_specs = (placed, plain_spec)
    return pl.pallas_call(
        functools.partial(conv_kernel, stage, len(stats)),
        grid_spec=pltpu.PrefetchScalarGridSpec(
            num_scalar_prefetch=1,
            grid=(chunks + 1,),
            in_specs=in_specs,
            out_specs=out_specs,
            scratch_shapes=[
                pltpu.VMEM((width, width), jnp.bfloat16),
                pltpu.VMEM((block, columns + 16, channels), jnp.float32),
                pltpu.VMEM((unit * columns, width), jnp.bfloat16),
                pltpu.VMEM((unit * columns, width), jnp.bfloat16),
                pltpu.VMEM((2, block * columns, width), jnp.float32),
                pltpu.VMEM((columns, channels), jnp.float32),
                pltpu.VMEM((columns, channels), jnp.float32),
                pltpu.VMEM((8, channels), jnp.float32),
                pltpu.SemaphoreType.DMA((1,)),
            ],
        ),
        out_shape=out_shape,
        input_output_aliases=aliases,
        compiler_params=pltpu.CompilerParams(
            vmem_limit_bytes=VMEM_LIMIT, dimension_semantics=("arbitrary",)
        ),
        cost_estimate=pl.CostEstimate(
            flops=2 * rows * columns * width * width,
            bytes_accessed=4 * rows * columns * channels,
            transcendentals=rows * columns * channels,
        ),
        name=f"conv{stage}",
    )(scal, *args)


def place_kernel(scal, a_ref, b_ref, _, out_ref):
    @pl.when(scal[0] == 0)
    def _():
        out_ref[...] = a_ref[...]

    @pl.when(scal[0] != 0)
    def _():
        out_ref[...] = b_ref[...]


def place(sample, count, scal, when_first, when_second, out):
    rows, columns, channels = out.shape[1:]
    block = pick_block(rows)
    tile = (1, block, columns, channels)
    return pl.pallas_call(
        place_kernel,
        grid_spec=pltpu.PrefetchScalarGridSpec(
            num_scalar_prefetch=1,
            grid=(rows // block,),
            in_specs=[
                pl.BlockSpec(tile, lambda c, scal: (0, jnp.where(scal[0] == 0, c, 0), 0, 0)),
                pl.BlockSpec(tile, lambda c, scal: (0, jnp.where(scal[0] == 0, 0, c), 0, 0)),
                pl.BlockSpec(memory_space=pl.ANY),
            ],
            out_specs=pl.BlockSpec(tile, lambda c, scal: ((1 - scal[0]) * count + sample, c, 0, 0)),
        ),
        out_shape=jax.ShapeDtypeStruct(out.shape, out.dtype),
        input_output_aliases={3: 0},
        compiler_params=pltpu.CompilerParams(vmem_limit_bytes=VMEM_LIMIT),
        cost_estimate=pl.CostEstimate(flops=0, bytes_accessed=4 * rows * columns * channels, transcendentals=0),
        name="place",
    )(scal, when_first, when_second, out)


def everyones(value):
    size = lax.axis_size("space")
    if size > 4:
        gathered = lax.all_gather(value, "space", axis=0)
        return [gathered[i] for i in range(size)]
    found = [value]
    for hop in range(1, size):
        found.append(lax.ppermute(value, "space", [(i, (i + hop) % size) for i in range(size)]))
    return found


def edge_rows(last, first):
    size = lax.axis_size("space")
    up = [(i, i + 1) for i in range(size - 1)]
    return lax.ppermute(last, "space", up), lax.ppermute(first, "space", [(j, i) for i, j in up])


def on_device(latents, kernels, norm_gain, norm_bias, conv_bias):
    section = lax.axis_index("section")
    space, spaces = lax.axis_index("space"), lax.axis_size("space")
    samples = latents.shape[0]
    count = samples // lax.axis_size("section")
    scal = jnp.stack([section, (space > 0).astype(jnp.int32), (space < spaces - 1).astype(jnp.int32), section * count])
    scal = scal.astype(jnp.int32)

    swap = [(0, 1), (1, 0)]
    own_w = pack_weights(kernels[0])
    other_w = lax.ppermute(own_w, "section", swap)
    own_p = jnp.concatenate([norm_gain, norm_bias, conv_bias, jnp.zeros((5, norm_gain.shape[1]), jnp.float32)])
    other_p = lax.ppermute(own_p, "section", swap)
    params = [jnp.where(section == stage, own_p, other_p) for stage in range(2)]

    edges = [
        lax.dynamic_slice(latents, (section * count, row, 0, 0), (count, 1) + latents.shape[2:])[:, 0]
        for row in (latents.shape[1] - 1, 0)
    ]
    tops, bottoms = edge_rows(*edges)
    stats = everyones(moments(scal, latents, count))

    firsts, halos, first_stats, arrived = [], [], [], []
    for s in range(count):
        first, own_stats = conv(0, s, scal, latents, tops[s], bottoms[s], stats, params[0], own_w, other_w)
        firsts.append(first)
        first_stats.append(everyones(own_stats))
        halos.append(edge_rows(first[0, -1], first[0, 0]))
        arrived.append(lax.ppermute(first, "section", [(1, 0)]))
    out, sent = None, []
    for s in range(count):
        out, second = conv(
            1, s, scal, firsts[s], *halos[s], first_stats[s], params[1], own_w, other_w, latents, out
        )
        sent.append(lax.ppermute(second, "section", [(0, 1)]))
    for s in range(count):
        out = place(s, count, scal, arrived[s], sent[s], out)
    return out[None]


def solution(mesh):
    return jax.shard_map(
        on_device,
        mesh=mesh,
        in_specs=(
            P("dp", "space", None, None),
            P("section", None, None, None, None),
            P("section", None),
            P("section", None),
            P("section", None),
        ),
        out_specs=P("section", "dp", "space", None, None),
        check_vma=False,
    )
```

```python
import functools

import jax
import jax.numpy as jnp
from jax import lax
from jax.experimental import pallas as pl
from jax.experimental.pallas import tpu as pltpu
from jax.sharding import PartitionSpec as P

GROUPS = 32
EPS = 1e-05
MAIN = 256
VMEM_LIMIT = 60 * 1024 * 1024


def pick_block(rows):
    return max(d for d in range(1, 9) if rows % d == 0)


def conv_block(rows):
    return max(d for d in range(1, 5) if rows % d == 0)


def column_pieces(channels):
    main = channels // MAIN * MAIN
    tail = channels - main
    return main, tail, 3 * main


def packed_width(channels):
    return -(-3 * channels // MAIN) * MAIN


def pack_kernel(k_ref, w_ref, buf):
    channels = k_ref.shape[-1]
    main, tail, base = column_pieces(channels)
    buf[...] = jnp.zeros_like(buf)
    for dr in range(3):
        for dc in range(3):
            tap = k_ref[dr, dc]
            for klo, khi, kdst in ((0, main, dc * main), (main, channels, base + dc * tail)):
                for nlo, nhi, ndst in ((0, main, dr * main), (main, channels, base + dr * tail)):
                    buf[kdst:kdst + khi - klo, ndst:ndst + nhi - nlo] = tap[klo:khi, nlo:nhi]
    w_ref[...] = buf[...]


def pack_weights(kernel):
    channels = kernel.shape[-1]
    width = packed_width(channels)
    return pl.pallas_call(
        pack_kernel,
        out_shape=jax.ShapeDtypeStruct((width, width), jnp.bfloat16),
        scratch_shapes=[pltpu.VMEM((width, width), jnp.bfloat16)],
        compiler_params=pltpu.CompilerParams(vmem_limit_bytes=VMEM_LIMIT),
        cost_estimate=pl.CostEstimate(flops=0, bytes_accessed=6 * width * width, transcendentals=0),
        name="pack",
    )(kernel)


def row_moments(values):
    mean = jnp.sum(values, axis=0, keepdims=True) * (1.0 / values.shape[0])
    deviation = values - mean
    return mean, jnp.sum(deviation * deviation, axis=0, keepdims=True)


def moments_kernel(scal, x_ref, m_ref):
    for i in range(x_ref.shape[1]):
        mean, spread = row_moments(x_ref[0, i].astype(jnp.float32))
        m_ref[0, 0, 0, i:i + 1, :] = mean
        m_ref[0, 1, 0, i:i + 1, :] = spread


def moments(scal, latents, count):
    _, rows, columns, channels = latents.shape
    block = pick_block(rows)
    return pl.pallas_call(
        moments_kernel,
        grid_spec=pltpu.PrefetchScalarGridSpec(
            num_scalar_prefetch=1,
            grid=(count, rows // block),
            in_specs=[
                pl.BlockSpec((1, block, columns, channels), lambda s, c, scal: (scal[3] + s, c, 0, 0))
            ],
            out_specs=pl.BlockSpec((1, 2, 1, block, channels), lambda s, c, scal: (s, 0, c, 0, 0)),
        ),
        out_shape=jax.ShapeDtypeStruct((count, 2, rows // block, block, channels), jnp.float32),
        compiler_params=pltpu.CompilerParams(vmem_limit_bytes=VMEM_LIMIT),
        cost_estimate=pl.CostEstimate(
            flops=0, bytes_accessed=count * rows * columns * channels * 2, transcendentals=0
        ),
        name="moments",
    )(scal, latents)


def stat_rows(ref, columns, rows):
    if len(ref.shape) == 2:
        return [(ref[columns:columns + rows, :], ref[columns + rows:columns + 2 * rows, :])]
    return [(ref[0, 0, j], ref[0, 1, j]) for j in range(ref.shape[2])]


def conv_kernel(stage, parts, *refs):
    scal, x_ref, top_ref, bot_ref = refs[:4]
    stat_refs = refs[4:4 + parts]
    par_ref, wa_ref, wb_ref = refs[4 + parts:7 + parts]
    rest = refs[7 + parts:]
    if stage == 0:
        y_ref, m_ref, up_ref, down_ref = rest[:4]
    else:
        res_ref, own_ref = rest[:2]
        keep_ref, y_ref = rest[-13:-11]
    w_ref, act_ref, lhs_a, lhs_b, p_a, p_b, edge_ref, carry_ref, next_ref, ab_ref = rest[-11:-1]
    sem = rest[-1]
    step, last = pl.program_id(0), pl.num_programs(0) - 1
    block, columns, channels = x_ref.shape[1:]
    main, tail, base = column_pieces(channels)
    width = w_ref.shape[0]

    @pl.when(step == 0)
    def _():
        own_first = scal[0] == stage
        copy_a = pltpu.make_async_copy(wa_ref, w_ref, sem.at[0])
        copy_b = pltpu.make_async_copy(wb_ref, w_ref, sem.at[0])

        @pl.when(own_first)
        def _():
            copy_a.start()

        @pl.when(jnp.logical_not(own_first))
        def _():
            copy_b.start()

        act_ref[:, 0:8, :] = jnp.zeros((act_ref.shape[0], 8, channels), jnp.float32)
        act_ref[:, columns + 8:columns + 16, :] = jnp.zeros((act_ref.shape[0], 8, channels), jnp.float32)
        per_group = channels // GROUPS
        row_id = lax.broadcasted_iota(jnp.int32, (channels, channels), 0).astype(jnp.float32)
        col_id = lax.broadcasted_iota(jnp.int32, (channels, channels), 1).astype(jnp.float32)
        same = jnp.floor((row_id + 0.5) * (1.0 / per_group)) == jnp.floor((col_id + 0.5) * (1.0 / per_group))
        members = jnp.where(same, 1.0, 0.0).astype(jnp.float32)

        def over_groups(value):
            return jnp.dot(
                jnp.broadcast_to(value, (8, channels)), members,
                precision=lax.Precision.HIGHEST, preferred_element_type=jnp.float32,
            )[0:1]

        rows = stat_refs[0].shape[2] * stat_refs[0].shape[3]
        cells = parts * rows
        total = jnp.zeros((1, channels), jnp.float32)
        for ref in stat_refs:
            for means, _ in stat_rows(ref, columns, rows):
                total += jnp.sum(means, axis=0, keepdims=True)
        mean = over_groups(total) * (1.0 / (cells * per_group))
        spread = jnp.zeros((1, channels), jnp.float32)
        for ref in stat_refs:
            for means, squares in stat_rows(ref, columns, rows):
                away = means - mean
                spread += jnp.sum(away * away * float(columns) + squares, axis=0, keepdims=True)
        var = over_groups(spread) * (1.0 / (cells * per_group * columns))
        inv = lax.rsqrt(var + EPS)
        ab_ref[0:1, :] = mean
        ab_ref[1:2, :] = 0.5 * inv * par_ref[0:1, :]
        ab_ref[2:3, :] = 0.5 * par_ref[1:2, :]
        copy_a.wait()

    def activate(values, slot, lhs, place, valid=None):
        half = (values.astype(jnp.float32) - ab_ref[0:1, :]) * ab_ref[1:2, :] + ab_ref[2:3, :]
        act = half + half * jnp.tanh(half)
        if valid is not None:
            act = jnp.where(valid, act, 0.0)
        act_ref[slot, 8:columns + 8, :] = act
        rows = slice(place * columns, (place + 1) * columns)
        for dc in range(3):
            lhs[rows, dc * main:(dc + 1) * main] = act_ref[slot, 7 + dc:7 + dc + columns, 0:main].astype(jnp.bfloat16)
        tails = [act_ref[slot, 7 + dc:7 + dc + columns, main:channels] for dc in range(3)]
        tails.append(jnp.zeros((columns, width - base - 3 * tail), jnp.float32))
        lhs[rows, base:width] = jnp.concatenate(tails, axis=1).astype(jnp.bfloat16)

    def edge(ref, valid, tap, dst):
        activate(ref[0:columns, :], 0, edge_ref, 0, valid)
        left = edge_ref[...]
        dst[:, 0:main] = jnp.dot(left, w_ref[:, tap * main:(tap + 1) * main], preferred_element_type=jnp.float32)
        ends = jnp.dot(left, w_ref[:, base:width], preferred_element_type=jnp.float32)
        dst[:, main:channels] = ends[:, tap * tail:(tap + 1) * tail]

    shift = par_ref[2:3, :]

    def tap_of(p, i, tap):
        rows = slice(i * columns, (i + 1) * columns)
        return (
            p[rows, tap * main:(tap + 1) * main],
            p[rows, base + tap * tail:base + (tap + 1) * tail],
        )

    def whole(ref):
        return ref[:, 0:main], ref[:, main:channels]

    def combine(p, i):
        chunk = jnp.maximum(step - 2, 0)
        above = whole(carry_ref) if i == 0 else tap_of(p, i - 1, 0)
        middle = tap_of(p, i, 1)
        below = whole(next_ref) if i == block - 1 else tap_of(p, i + 1, 2)
        for j, (lo, hi) in enumerate(((0, main), (main, channels))):
            total = above[j] + middle[j] + below[j] + shift[:, lo:hi]
            if stage == 1:
                total = total + res_ref[0, i, :, lo:hi].astype(jnp.float32)
            rounded = total.astype(jnp.bfloat16)
            y_ref[0, i, :, lo:hi] = rounded
            if stage == 0:
                mean, spread = row_moments(rounded.astype(jnp.float32))
                m_ref[0, 0, chunk, i:i + 1, lo:hi] = mean
                m_ref[0, 1, chunk, i:i + 1, lo:hi] = spread
            else:
                keep_ref[0, i, :, lo:hi] = jnp.where(scal[0] == 0, own_ref[0, i, :, lo:hi], rounded)

    def save_carry(p):
        left, right = tap_of(p, block - 1, 0)
        carry_ref[:, 0:main] = left
        carry_ref[:, main:channels] = right

    @pl.when(step == 0)
    def _():
        for i in range(block):
            activate(x_ref[0, i], i, lhs_a, i)

    @pl.when(step == 2)
    def _():
        edge(top_ref, scal[1] == 1, 0, carry_ref)

    def turn(lhs_now, lhs_next, p_now, p_before):
        pieces = width // MAIN
        for n in range(pieces):
            cols = slice(n * MAIN, (n + 1) * MAIN)
            p_now[:, cols] = jnp.dot(lhs_now[...], w_ref[:, cols], preferred_element_type=jnp.float32)
            for i in range(n * block // pieces, (n + 1) * block // pieces):
                activate(x_ref[0, i], i, lhs_next, i)
                if i < block - 1:
                    combine(p_before, i)
        left, right = tap_of(p_now, 0, 2)
        next_ref[:, 0:main] = left
        next_ref[:, main:channels] = right
        combine(p_before, block - 1)
        save_carry(p_before)

    middle_step = jnp.logical_and(step > 0, step < last)

    @pl.when(jnp.logical_and(middle_step, step % 2 == 1))
    def _():
        turn(lhs_a, lhs_b, p_a, p_b)

    @pl.when(jnp.logical_and(middle_step, step % 2 == 0))
    def _():
        turn(lhs_b, lhs_a, p_b, p_a)

    if stage == 0:
        @pl.when(step == 2)
        def _():
            down_ref[0:columns, :] = y_ref[0, 0].astype(jnp.float32)

    @pl.when(step == last)
    def _():
        edge(bot_ref, scal[2] == 1, 2, next_ref)
        for parity, p in ((1, p_a), (0, p_b)):
            @pl.when((last - 1) % 2 == parity)
            def _():
                for i in range(block):
                    combine(p, i)
        if stage == 0:
            if m_ref.shape[2] == 1:
                down_ref[0:columns, :] = y_ref[0, 0].astype(jnp.float32)
            up_ref[0:columns, :] = y_ref[0, block - 1].astype(jnp.float32)
            for j in range(m_ref.shape[2]):
                for q in range(2):
                    at = columns + (q * m_ref.shape[2] + j) * block
                    for ref in (up_ref, down_ref):
                        ref[at:at + block, :] = m_ref[0, q, j]


def conv(stage, sample, scal, source, top, bottom, stats, params, own, other, latents=None, out=None):
    rows, columns, channels = source.shape[1:]
    block = conv_block(rows)
    chunks = rows // block
    width = packed_width(channels)
    tile = (1, block, columns, channels)
    lag = lambda c: jnp.clip(c - 2, 0, chunks - 1)
    ahead = lambda c: jnp.minimum(c, chunks - 1)
    full = lambda a: pl.BlockSpec(a.shape, lambda c, scal, n=a.ndim: (0,) * n)
    anywhere = pl.BlockSpec(memory_space=pl.ANY)
    if stage == 0:
        main_spec = pl.BlockSpec(tile, lambda c, scal: (scal[3] + sample, ahead(c), 0, 0))
    else:
        main_spec = pl.BlockSpec(tile, lambda c, scal: (0, ahead(c), 0, 0))
    args = [source, top, bottom, *stats, params, own, other]
    in_specs = [main_spec, full(top), full(bottom), *[
        full(s) if s.ndim == 2 else pl.BlockSpec(
            (1,) + s.shape[1:], lambda c, scal: ((sample if stage == 0 else 0), 0, 0, 0, 0)
        ) for s in stats
    ], full(params), anywhere, anywhere]
    plain = jax.ShapeDtypeStruct((1, rows, columns, channels), jnp.bfloat16)
    plain_spec = pl.BlockSpec(tile, lambda c, scal: (0, lag(c), 0, 0))
    aliases = {}
    if stage == 0:
        moment = jax.ShapeDtypeStruct((1, 2, chunks, block, channels), jnp.float32)
        message = jax.ShapeDtypeStruct((columns + 2 * rows, channels), jnp.float32)
        out_shape = (plain, moment, message, message)
        out_specs = (plain_spec, full(jnp.zeros(moment.shape)), full(jnp.zeros(message.shape)), full(jnp.zeros(message.shape)))
    else:
        placed = pl.BlockSpec(tile, lambda c, scal: (scal[3] + sample, lag(c), 0, 0))
        args += [latents, source]
        in_specs += [placed, plain_spec]
        if out is not None:
            args.append(out)
            in_specs.append(anywhere)
            aliases = {len(args): 0}
        out_shape = (jax.ShapeDtypeStruct(latents.shape, jnp.bfloat16), plain)
        out_specs = (placed, plain_spec)
    return pl.pallas_call(
        functools.partial(conv_kernel, stage, len(stats)),
        grid_spec=pltpu.PrefetchScalarGridSpec(
            num_scalar_prefetch=1,
            grid=(chunks + 2,),
            in_specs=in_specs,
            out_specs=out_specs,
            scratch_shapes=[
                pltpu.VMEM((width, width), jnp.bfloat16),
                pltpu.VMEM((block, columns + 16, channels), jnp.float32),
                pltpu.VMEM((block * columns, width), jnp.bfloat16),
                pltpu.VMEM((block * columns, width), jnp.bfloat16),
                pltpu.VMEM((block * columns, width), jnp.float32),
                pltpu.VMEM((block * columns, width), jnp.float32),
                pltpu.VMEM((columns, width), jnp.bfloat16),
                pltpu.VMEM((columns, channels), jnp.float32),
                pltpu.VMEM((columns, channels), jnp.float32),
                pltpu.VMEM((8, channels), jnp.float32),
                pltpu.SemaphoreType.DMA((1,)),
            ],
        ),
        out_shape=out_shape,
        input_output_aliases=aliases,
        compiler_params=pltpu.CompilerParams(
            vmem_limit_bytes=VMEM_LIMIT, dimension_semantics=("arbitrary",)
        ),
        cost_estimate=pl.CostEstimate(
            flops=2 * rows * columns * width * width,
            bytes_accessed=4 * rows * columns * channels,
            transcendentals=rows * columns * channels,
        ),
        name=f"conv{stage}",
    )(scal, *args)


def place_kernel(scal, a_ref, b_ref, _, out_ref):
    @pl.when(scal[0] == 0)
    def _():
        out_ref[...] = a_ref[...]

    @pl.when(scal[0] != 0)
    def _():
        out_ref[...] = b_ref[...]


def place(sample, count, scal, when_first, when_second, out):
    rows, columns, channels = out.shape[1:]
    block = pick_block(rows)
    tile = (1, block, columns, channels)
    return pl.pallas_call(
        place_kernel,
        grid_spec=pltpu.PrefetchScalarGridSpec(
            num_scalar_prefetch=1,
            grid=(rows // block,),
            in_specs=[
                pl.BlockSpec(tile, lambda c, scal: (0, jnp.where(scal[0] == 0, c, 0), 0, 0)),
                pl.BlockSpec(tile, lambda c, scal: (0, jnp.where(scal[0] == 0, 0, c), 0, 0)),
                pl.BlockSpec(memory_space=pl.ANY),
            ],
            out_specs=pl.BlockSpec(tile, lambda c, scal: ((1 - scal[0]) * count + sample, c, 0, 0)),
        ),
        out_shape=jax.ShapeDtypeStruct(out.shape, out.dtype),
        input_output_aliases={3: 0},
        compiler_params=pltpu.CompilerParams(vmem_limit_bytes=VMEM_LIMIT),
        cost_estimate=pl.CostEstimate(flops=0, bytes_accessed=4 * rows * columns * channels, transcendentals=0),
        name="place",
    )(scal, when_first, when_second, out)


def everyones(value):
    size = lax.axis_size("space")
    if size > 4:
        gathered = lax.all_gather(value, "space", axis=0)
        return [gathered[i] for i in range(size)]
    found = [value]
    for hop in range(1, size):
        found.append(lax.ppermute(value, "space", [(i, (i + hop) % size) for i in range(size)]))
    return found


def edge_rows(last, first):
    size = lax.axis_size("space")
    up = [(i, i + 1) for i in range(size - 1)]
    return lax.ppermute(last, "space", up), lax.ppermute(first, "space", [(j, i) for i, j in up])


def on_device(latents, kernels, norm_gain, norm_bias, conv_bias):
    section = lax.axis_index("section")
    space, spaces = lax.axis_index("space"), lax.axis_size("space")
    samples = latents.shape[0]
    count = samples // lax.axis_size("section")
    scal = jnp.stack([section, (space > 0).astype(jnp.int32), (space < spaces - 1).astype(jnp.int32), section * count])
    scal = scal.astype(jnp.int32)

    swap = [(0, 1), (1, 0)]
    own_w = pack_weights(kernels[0])
    other_w = lax.ppermute(own_w, "section", swap)
    own_p = jnp.concatenate([norm_gain, norm_bias, conv_bias, jnp.zeros((5, norm_gain.shape[1]), jnp.float32)])
    other_p = lax.ppermute(own_p, "section", swap)
    params = [jnp.where(section == stage, own_p, other_p) for stage in range(2)]

    edges = [
        lax.dynamic_slice(latents, (section * count, row, 0, 0), (count, 1) + latents.shape[2:])[:, 0]
        for row in (latents.shape[1] - 1, 0)
    ]
    tops, bottoms = edge_rows(*edges)
    stats = everyones(moments(scal, latents, count))

    firsts, halos, first_stats, arrived = [], [], [], []
    for s in range(count):
        first, own_stats, up, down = conv(
            0, s, scal, latents, tops[s], bottoms[s], stats, params[0], own_w, other_w
        )
        firsts.append(first)
        if 3 <= spaces <= 4:
            ring = lambda hop: [(i, (i + hop) % spaces) for i in range(spaces)]
            above, below = (lax.ppermute(up, "space", ring(1)), lax.ppermute(down, "space", ring(spaces - 1)))
            others = [lax.ppermute(own_stats, "space", ring(hop)) for hop in range(2, spaces - 1)]
            first_stats.append([own_stats, above, below, *others])
            halos.append((above, below))
        else:
            first_stats.append(everyones(own_stats))
            columns = latents.shape[2]
            halos.append(edge_rows(up[0:columns], down[0:columns]))
        arrived.append(lax.ppermute(first, "section", [(1, 0)]))
    out, sent = None, []
    for s in range(count):
        out, second = conv(
            1, s, scal, firsts[s], *halos[s], first_stats[s], params[1], own_w, other_w, latents, out
        )
        sent.append(lax.ppermute(second, "section", [(0, 1)]))
    for s in range(count):
        out = place(s, count, scal, arrived[s], sent[s], out)
    return out[None]


def solution(mesh):
    return jax.shard_map(
        on_device,
        mesh=mesh,
        in_specs=(
            P("dp", "space", None, None),
            P("section", None, None, None, None),
            P("section", None),
            P("section", None),
            P("section", None),
        ),
        out_specs=P("section", "dp", "space", None, None),
        check_vma=False,
    )
```
